32 devices in a mesh: row: 8 (over z, y), col: 4 (over x, core).
Axes of the slice: x: 2, y: 2, z: 4, core: 2. Of those that a mesh axis runs over, the one named last changes fastest.
Arguments:
- root_rhs: bfloat16 [8, 8192], replicated, may hold values from -6 to 6
- diag_inv: bfloat16 [16, 512, 512], replicated, may hold values from -1 to 2
- tile_u: bfloat16 [8, 4, 2, 4, 128, 512], P('row', 'col'), may hold values from -0.1875 to 0.1875
- tile_v: bfloat16 [8, 4, 2, 4, 512, 128], P('row', 'col'), may hold values from -0.25 to 0.25
- tile_rank: int32 [8, 4, 2, 4], P('row', 'col'), may hold values from 16 to 128
- child_x: bfloat16 [32, 8, 512], P(('row', 'col')), may hold values from -6 to 6
- border_t: bfloat16 [32, 512, 1024], P(('row', 'col')), may hold values from -0.09375 to 0.09375
- child_inv: bfloat16 [32, 512, 512], P(('row', 'col')), may hold values from -1 to 2
- child_blocks: int32 [32, 8], P(('row', 'col')), may hold values from 0 to 63
Outputs:
- root_solution: float32 [8, 8192], P(None, ('row', 'col'))
- child_out: float32 [32, 8, 512], P(('row', 'col'))
The draws below stay inside these ranges and needn't reach their ends.
All inputs are finite; a program needn't handle non-finite values.
Results may differ from the reference program's by a relative error of at most 0.017.
Values sent between devices are 32-bit elements; how exact they have to be, the bound alone decides.
A program may use at most 64 MiB of HBM per device.

```python
import math
import jax
import jax.numpy as jnp
import numpy as np
from jax import lax

NT = 16
TILE = 512
RHS = 8
RMAX = 128
BLK = 128
BB = 8
CSEP = 512
F = 8192
NB = 64
BORD = 1024
TR = 2
TC = 4
CHILDREN = 32
N_ROW = 8
N_COL = 4


def inverse_blocks(key, count, order):
    first, second_operand = jax.random.split(key, 2)
    diagonal = jax.random.uniform(first, (count, order), jnp.float32, 0.6, 1.2)
    spread = jnp.clip(jax.random.normal(second_operand, (count, order, order), jnp.float32), -6.0, 6.0)
    identity = jnp.eye(order, dtype=jnp.float32)
    blocks = spread * (0.5 / math.sqrt(order)) * (1.0 - identity) + identity[None] * diagonal[:, :, None]
    return blocks.astype(jnp.bfloat16)


def draw_diag_inv(key, part):
    return inverse_blocks(jax.random.fold_in(key, 11), NT, TILE)


def draw_child_inv(key, part):
    return inverse_blocks(jax.random.fold_in(key, 23), CHILDREN, CSEP)


def set_ends(entries, own_key, smallest, high):
    index_at = [jax.random.randint(jax.random.fold_in(own_key, axis), (), 0, length) for axis, length in enumerate(entries.shape)]
    longest = entries.shape.index(max(entries.shape))
    neighbour = index_at[:longest] + [(index_at[longest] + 1) % entries.shape[longest]] + index_at[longest + 1:]
    return entries.at[tuple(index_at)].set(smallest).at[tuple(neighbour)].set(high)


def block_scale(own_key, extent, cuts, least, high):
    def one(position, shards_of):
        steps = jax.random.uniform(jax.random.fold_in(jax.random.fold_in(own_key, 6), position), (shards_of,), jnp.float32, least / len(cuts), high / len(cuts))
        return jnp.repeat(jnp.exp(steps), extent[position] // shards_of).reshape((-1,) + (1,) * (len(extent) - position - 1))

    factor_of = one(*cuts[0])
    for cut in cuts[1:]:
        factor_of = factor_of * one(*cut)
    return factor_of


def rank_bounds(number_of, slope):
    weights = [(1 << 20) // math.isqrt(standing ** slope) + 1 for standing in range(1, number_of + 1)]
    scale = 1 + sum(weights) // (1 << 30)
    return np.cumsum(np.array([max(1, weight // scale) for weight in weights]))


def ranked(own_key, dims, amount, slope):
    table = rank_bounds(amount, slope)
    lot = jax.random.randint(jax.random.fold_in(own_key, 1), dims, 0, int(table[amount - 1]))
    standing = jnp.searchsorted(jnp.asarray(table, jnp.int32), lot, side="right")
    return jax.random.permutation(jax.random.fold_in(own_key, 2), amount)[standing].astype(jnp.int32)


def normal_values(stream_key, shape, scale, reach, cuts=(), kind=jnp.bfloat16):
    values = scale * jax.random.normal(stream_key, shape, jnp.float32)
    if cuts:
        values = values * block_scale(stream_key, shape, cuts, -0.22, 0.18)
    return jnp.clip(values, -reach, reach).astype(kind)


def setup_inputs(seed: int = 0) -> dict:
    splits = jax.random.split(jax.random.key(seed), 10)
    return {
        "root_rhs": normal_values(splits[0], (RHS, F), 1.0, 6.0),
        "diag_inv": draw_diag_inv(jax.random.fold_in(splits[9], 71), 0),
        "tile_u": normal_values(splits[2], (N_ROW, N_COL, TR, TC, RMAX, TILE), (RMAX * NT // 2) ** -0.5, 0.1875, ((0, 8), (1, 4))),
        "tile_v": normal_values(splits[3], (N_ROW, N_COL, TR, TC, TILE, RMAX), TILE ** -0.5, 0.25, ((0, 8), (1, 4))),
        "tile_rank": set_ends(jax.random.randint(splits[4], (N_ROW, N_COL, TR, TC), RMAX // 8, RMAX + 1), jax.random.fold_in(splits[4], 1), RMAX // 8, RMAX).astype(jnp.int32),
        "child_x": normal_values(splits[5], (CHILDREN, RHS, CSEP), 1.0, 6.0, ((0, 32),)),
        "border_t": normal_values(splits[6], (CHILDREN, CSEP, BORD), (CSEP * BB) ** -0.5, 0.09375, ((0, 32),)),
        "child_inv": draw_child_inv(jax.random.fold_in(splits[9], 71), 0),
        "child_blocks": set_ends(ranked(splits[8], (CHILDREN, BB), NB, 1), jax.random.fold_in(splits[8], 3), 0, NB - 1).astype(jnp.int32),
    }


def rounded_value(values):
    return lax.optimization_barrier(values.astype(jnp.bfloat16)).astype(jnp.float32)


def reference(root_rhs, diag_inv, tile_u, tile_v, tile_rank, child_x, border_t, child_inv, child_blocks):
    highest_precision = lax.Precision.HIGHEST
    upward = jnp.einsum('crs,csb->crb', child_x.astype(jnp.float32), border_t.astype(jnp.float32))
    pieces = upward.reshape(CHILDREN, RHS, BB, BLK).transpose(1, 0, 2, 3).reshape(RHS, CHILDREN * BB, BLK)
    flat_blocks = child_blocks.reshape(-1).astype(jnp.int32)
    dense_sum = jnp.zeros((RHS, NB, BLK), jnp.float32).at[:, flat_blocks, :].add(pieces)
    child_sum = dense_sum.reshape(RHS, NT, TILE)
    right_side = root_rhs.astype(jnp.float32).reshape(RHS, NT, TILE)
    inverses = diag_inv.astype(jnp.float32)
    rank_iota = jnp.arange(RMAX)
    tile_ids = jnp.arange(NT)
    solved_rows = jnp.zeros((RHS, NT, TILE), jnp.float32)
    for column in range(NT):
        owner_row, owner_slot = column % N_ROW, column // N_ROW
        left_rows = tile_u[owner_row, :, owner_slot].transpose(1, 0, 2, 3).reshape(NT, RMAX, TILE)
        right_row_indices = tile_v[owner_row, :, owner_slot].transpose(1, 0, 2, 3).reshape(NT, TILE, RMAX)
        rank_rows = tile_rank[owner_row, :, owner_slot].T.reshape(NT)
        live_mask = (rank_iota[None, :] < rank_rows[:, None]) & (tile_ids[:, None] < column)
        coefficient_values = jnp.einsum('gic,icw->giw', rounded_value(solved_rows), right_row_indices.astype(jnp.float32))
        coefficient_values = rounded_value(jnp.where(live_mask[None], coefficient_values, 0.0))
        partial_value = jnp.einsum('rkq,kqt->rt', coefficient_values, left_rows.astype(jnp.float32))
        row_total = partial_value + child_sum[:, column]
        fresh = jnp.dot(right_side[:, column] - row_total, inverses[column], precision=highest_precision)
        solved_rows = solved_rows.at[:, column].set(fresh)
    result = jnp.zeros((RHS, NT, TILE), jnp.float32)
    for column in reversed(range(NT)):
        owner_col, owner_slot = column % N_COL, column // N_COL
        left_cols = tile_u[:, owner_col, :, owner_slot].transpose(1, 0, 2, 3).reshape(NT, RMAX, TILE)
        right_cols = tile_v[:, owner_col, :, owner_slot].transpose(1, 0, 2, 3).reshape(NT, TILE, RMAX)
        rank_cols = tile_rank[:, owner_col, :, owner_slot].T.reshape(NT)
        live_mask = (rank_iota[None, :] < rank_cols[:, None]) & (tile_ids[:, None] > column)
        coefficient_values = jnp.einsum('rit,iqt->riq', rounded_value(result), left_cols.astype(jnp.float32))
        coefficient_values = rounded_value(jnp.where(live_mask[None], coefficient_values, 0.0))
        partial_value = jnp.einsum('riq,itq->rt', coefficient_values, right_cols.astype(jnp.float32))
        fresh = jnp.dot(solved_rows[:, column] - partial_value, inverses[column].T, precision=highest_precision)
        result = result.at[:, column].set(fresh)
    root_solution = result.reshape(RHS, F)
    gathered = result.reshape(RHS, NB, BLK)[:, flat_blocks, :].reshape(RHS, CHILDREN, BB * BLK)
    returned = jnp.einsum('rcb,csb->crs', rounded_value(gathered), border_t.astype(jnp.float32))
    child_out = child_x.astype(jnp.float32) - jnp.einsum('crs,cst->crt', returned, child_inv.astype(jnp.float32), precision=highest_precision)
    return root_solution, child_out
```

```python
import functools
import jax
import jax.numpy as jnp
from jax import lax
from jax.experimental import pallas as pl
from jax.experimental.pallas import tpu as pltpu
from jax.sharding import PartitionSpec as P

BLK = 128
F32 = jnp.float32
BF16 = jnp.bfloat16
MESH = pl.DeviceIdType.MESH
NN = (((1,), (0,)), ((), ()))
NT = (((1,), (1,)), ((), ()))


def dot(a, b, dims=NN):
    return lax.dot_general(a, b, dims, preferred_element_type=F32)


def two_part(a):
    high = a.astype(BF16).astype(F32)
    return jnp.concatenate([high, a - high], axis=0).astype(BF16)


def wide_dot(a, b, dims=NN):
    n = a.shape[0]
    both = dot(two_part(a), b, dims)
    return both[:n] + both[n:]


def solve_kernel(
    n_row, n_col, t_rows, t_cols, ntile, n_child, bb, share,
    rhs_hbm, dinv_hbm, u_hbm, v_hbm, rank_ref, cx_ref, bt_hbm, ci_hbm, cb_ref,
    root_out, child_out,
    rhs, drow, dcol, u, v, bt, ci, w, y,
    csum, csum_in, acc, fpart, xs, bacc, bpart, z_all,
    load_sem, csend, crecv, fsend, frecv, bsend, brecv, zsend, zrecv,
):
    r = lax.axis_index("row")
    c = lax.axis_index("col")
    n_dev = n_row * n_col
    me = r * n_col + c
    rhs_count, tile = acc.shape[1], acc.shape[2]
    rank_max = u.shape[2]
    per = tile // BLK
    i_max = r + n_row * (t_rows - 1)

    barrier = pltpu.get_barrier_semaphore()

    def greet(o, carry):
        other = lax.rem(me + o, n_dev)
        pl.semaphore_signal(
            barrier, inc=1, device_id=(other // n_col, lax.rem(other, n_col)), device_id_type=MESH
        )
        return carry

    lax.fori_loop(1, n_dev, greet, 0)

    loads = []

    def load(src, dst):
        copy = pltpu.make_async_copy(src, dst, load_sem.at[len(loads)])
        loads.append(copy)
        copy.start()
        return copy

    bt_load = load(bt_hbm, bt)
    row_loads = [load(dinv_hbm.at[r + n_row * a], drow.at[a]) for a in range(t_rows)]
    row_loads += [
        load(rhs_hbm.at[:, pl.ds(pl.multiple_of((r + n_row * a) * tile, tile), tile)], rhs.at[a])
        for a in range(t_rows)
    ]
    u_load = load(u_hbm, u)
    v_load = load(v_hbm, v)
    col_loads = [load(dinv_hbm.at[c + n_col * b], dcol.at[b]) for b in range(t_cols)]
    ci_load = load(ci_hbm, ci)

    for b in range(t_cols):
        bacc[b] = jnp.zeros((rhs_count, tile), F32)

    def need(row, k):
        return (row + n_row * (t_rows - 1) > k) | (row == lax.rem(k, n_row))

    for a in range(t_rows):
        for rr in range(n_row):
            @pl.when(jnp.logical_not(need(rr, r + n_row * a)))
            def _():
                bpart[a, rr] = jnp.zeros((rhs_count, tile), F32)

    bt_load.wait()
    ups = []
    for ch in range(n_child):
        up = dot(cx_ref[ch], bt[ch])
        ups.append([up[:, m * BLK:(m + 1) * BLK] for m in range(bb)])

    def spread(j, carry):
        row = lax.rem(j, n_row)
        slot = j // n_row
        for q in range(per):
            total = jnp.zeros((rhs_count, BLK), F32)
            for ch in range(n_child):
                for m in range(bb):
                    hit = jnp.where(cb_ref[ch, m] == j * per + q, 1.0, 0.0).astype(F32)
                    total = total + ups[ch][m] * hit
            csum[row, slot, :, q * BLK:(q + 1) * BLK] = total
        return carry

    lax.fori_loop(0, ntile, spread, 0)
    pl.semaphore_wait(barrier, n_dev - 1)

    def csum_copy(rr, slot):
        return pltpu.make_async_remote_copy(
            src_ref=csum.at[rr], dst_ref=csum_in.at[slot],
            send_sem=csend.at[rr], recv_sem=crecv.at[slot],
            device_id=(rr, c), device_id_type=MESH,
        )

    def csum_start(o, carry):
        csum_copy(lax.rem(r + o, n_row), r).start()
        return carry

    lax.fori_loop(1, n_row, csum_start, 0)

    for copy in row_loads:
        copy.wait()
    u_load.wait()

    def fold_left(t, carry):
        a = t // t_cols
        b = lax.rem(t, t_cols)
        full = dot(u[a, b], drow[a])
        high = full.astype(BF16)
        w[a, b, :rank_max] = high
        w[a, b, rank_max:] = (full - high.astype(F32)).astype(BF16)
        return carry

    lax.fori_loop(0, t_rows * t_cols, fold_left, 0)

    def csum_wait(o, carry):
        rr = lax.rem(r + o, n_row)
        csum_copy(rr, rr).wait_recv()
        return carry

    lax.fori_loop(1, n_row, csum_wait, 0)
    for a in range(t_rows):
        base = -csum[r, a]
        for o in range(1, n_row):
            base = base - csum_in[lax.rem(r + o, n_row), a]
        base = base + rhs[a].astype(F32) * jnp.where(c == 0, 1.0, 0.0).astype(F32)
        acc[a] = wide_dot(base, drow[a])

    def row_copy(a, rr, slot_b, slot_c, target_col):
        return pltpu.make_async_remote_copy(
            src_ref=acc.at[a], dst_ref=fpart.at[slot_b, slot_c],
            send_sem=fsend.at[a, rr], recv_sem=frecv.at[slot_b, slot_c],
            device_id=(rr, target_col), device_id_type=MESH,
        )

    def each_row_copy(a, act, own):
        i = r + n_row * a
        slot_b = i // n_col
        target = lax.rem(i, n_col)

        def one(t, carry):
            rr = lax.rem(r + t, n_row)

            @pl.when(need(rr, i))
            def _():
                act(row_copy(a, rr, slot_b, c, target))

            return carry

        lax.fori_loop(1, n_row, one, 0)

        @pl.when(target != c)
        def _():
            act(row_copy(a, r, slot_b, c, target))

        if own:
            @pl.when(target == c)
            def _():
                fpart[slot_b, c] = acc[a]

    def send_row(a):
        each_row_copy(a, lambda copy: copy.start(), True)

    def col_copy(b, cc, slot_a, slot_r, target_row):
        return pltpu.make_async_remote_copy(
            src_ref=bacc.at[b], dst_ref=bpart.at[slot_a, slot_r],
            send_sem=bsend.at[b, cc], recv_sem=brecv.at[slot_a, slot_r],
            device_id=(target_row, cc), device_id_type=MESH,
        )

    def each_col_copy(b, act, own):
        j = c + n_col * b
        slot_a = j // n_row
        target = lax.rem(j, n_row)
        for t in range(1, n_col):
            act(col_copy(b, lax.rem(c + n_col - t, n_col), slot_a, r, target))

        @pl.when(target != r)
        def _():
            act(col_copy(b, c, slot_a, r, target))

        if own:
            @pl.when(target == r)
            def _():
                bpart[slot_a, r] = bacc[b]

    def send_col(b):
        each_col_copy(b, lambda copy: copy.start(), True)

    lanes = lax.broadcasted_iota(jnp.int32, (rhs_count, rank_max), 1)

    def live(value, a, b):
        kept = jnp.where(lanes < rank_ref[a, b], value, 0.0).astype(BF16)
        return jnp.concatenate([kept, kept], axis=1)

    for a in range(t_rows):
        @pl.when(r + n_row * a <= c)
        def _():
            send_row(a)

    v_load.wait()
    for copy in col_loads:
        copy.wait()

    def forward(b, carry):
        k = c + n_col * b
        k_row = lax.rem(k, n_row)

        @pl.when(need(r, k))
        def _():
            for cc in range(n_col):
                @pl.when(jnp.logical_not((r == k_row) & (c == cc)))
                def _():
                    row_copy(0, lax.rem(r + 1, n_row), b, cc, c).wait_recv()

            x = fpart[b, 0]
            for cc in range(1, n_col):
                x = x + fpart[b, cc]
            xs[b] = x
            xb = x.astype(BF16)
            for a in range(t_rows):
                i = r + n_row * a

                @pl.when(i > k)
                def _():
                    p = live(dot(xb, v[a, b]), a, b)
                    acc[a] = acc[a] - dot(p, w[a, b])

                    @pl.when(i <= k + n_col)
                    def _():
                        send_row(a)

            @pl.when(r == k_row)
            def _():
                bacc[b] = wide_dot(xs[b], drow[k // n_row], NT)

                @pl.when(k >= i_max)
                def _():
                    send_col(b)

        @pl.when(b == 0)
        def _():
            def fold_right(t, inner):
                a = t // t_cols
                bq = lax.rem(t, t_cols)
                full = dot(dcol[bq], v[a, bq])
                high = full.astype(BF16)
                y[a, bq, :, :rank_max] = high
                y[a, bq, :, rank_max:] = (full - high.astype(F32)).astype(BF16)
                return inner

            lax.fori_loop(0, t_rows * t_cols, fold_right, 0)

        return carry

    lax.fori_loop(0, t_cols, forward, 0)

    def z_copy(a, rr, i):
        part = z_all.at[pl.ds(i * per, per)]
        return pltpu.make_async_remote_copy(
            src_ref=part, dst_ref=part, send_sem=zsend.at[a, rr], recv_sem=zrecv.at[i],
            device_id=(rr, c), device_id_type=MESH,
        )

    for a in reversed(range(t_rows)):
        i = r + n_row * a
        i_col = lax.rem(i, n_col)

        def wait_part(rr, carry):
            @pl.when(need(rr, i) & jnp.logical_not((rr == r) & (c == i_col)))
            def _():
                col_copy(0, lax.rem(c + 1, n_col), a, rr, r).wait_recv()

            return carry

        lax.fori_loop(0, n_row, wait_part, 0)
        z = bpart[a, 0]
        for rr in range(1, n_row):
            z = z + bpart[a, rr]
        for q in range(per):
            z_all[i * per + q] = z[:, q * BLK:(q + 1) * BLK]
        zb = z.astype(BF16)

        def back(t, carry):
            b = t_cols - 1 - t
            j = c + n_col * b

            @pl.when(j < i)
            def _():
                q = live(dot(zb, u[a, b], NT), a, b)
                bacc[b] = bacc[b] - dot(q, y[a, b], NT)

                @pl.when(j >= i - n_row)
                def _():
                    send_col(b)

            return carry

        lax.fori_loop(0, t_cols, back, 0)

        def z_start(o, carry):
            z_copy(a, lax.rem(r + o, n_row), i).start()
            return carry

        lax.fori_loop(1, n_row, z_start, 0)

    def z_wait(j, carry):
        @pl.when(lax.rem(j, n_row) != r)
        def _():
            z_copy(0, lax.rem(r + 1, n_row), j).wait_recv()

        return carry

    lax.fori_loop(0, ntile, z_wait, 0)

    if share % BLK == 0:
        for q in range(share // BLK):
            root_out[:, q * BLK:(q + 1) * BLK] = z_all[me * (share // BLK) + q]
    else:
        first = (me * share) // BLK
        root_out[...] = z_all[first]
    ci_load.wait()
    for ch in range(n_child):
        taken = jnp.concatenate([z_all[cb_ref[ch, m]] for m in range(bb)], axis=1).astype(BF16)
        returned = dot(taken, bt[ch], NT)
        child_out[ch] = cx_ref[ch].astype(F32) - wide_dot(returned, ci[ch])

    def csum_done(o, carry):
        csum_copy(lax.rem(r + o, n_row), r).wait_send()
        return carry

    lax.fori_loop(1, n_row, csum_done, 0)
    for a in range(t_rows):
        each_row_copy(a, lambda copy: copy.wait_send(), False)

        def z_done(o, carry):
            z_copy(a, lax.rem(r + o, n_row), r + n_row * a).wait_send()
            return carry

        lax.fori_loop(1, n_row, z_done, 0)
    for b in range(t_cols):
        @pl.when(need(r, c + n_col * b))
        def _():
            each_col_copy(b, lambda copy: copy.wait_send(), False)


def per_device(
    root_rhs, diag_inv, tile_u, tile_v, tile_rank, child_x, border_t, child_inv, child_blocks
):
    n_row = lax.axis_size("row")
    n_col = lax.axis_size("col")
    ntile, tile = diag_inv.shape[0], diag_inv.shape[1]
    rhs_count = root_rhs.shape[0]
    t_rows, t_cols, rank_max = tile_u.shape[2], tile_u.shape[3], tile_u.shape[4]
    n_child, bb = child_blocks.shape
    share = ntile * tile // (n_row * n_col)
    width = share if share % BLK == 0 else BLK
    vec = (rhs_count, tile)
    any_spec = pl.BlockSpec(memory_space=pl.ANY)
    vmem = pl.BlockSpec(memory_space=pltpu.VMEM)
    smem = pl.BlockSpec(memory_space=pltpu.SMEM)
    dma = pltpu.SemaphoreType.DMA
    root, child = pl.pallas_call(
        functools.partial(
            solve_kernel, n_row, n_col, t_rows, t_cols, ntile, n_child, bb, share
        ),
        out_shape=(
            jax.ShapeDtypeStruct((rhs_count, width), F32),
            jax.ShapeDtypeStruct(child_x.shape, F32),
        ),
        in_specs=[any_spec, any_spec, any_spec, any_spec, smem, vmem, any_spec, any_spec, smem],
        out_specs=(vmem, vmem),
        scratch_shapes=[
            pltpu.VMEM((t_rows,) + vec, BF16),
            pltpu.VMEM((t_rows, tile, tile), BF16),
            pltpu.VMEM((t_cols, tile, tile), BF16),
            pltpu.VMEM(tile_u.shape[2:], BF16),
            pltpu.VMEM(tile_v.shape[2:], BF16),
            pltpu.VMEM(border_t.shape, BF16),
            pltpu.VMEM(child_inv.shape, BF16),
            pltpu.VMEM((t_rows, t_cols, 2 * rank_max, tile), BF16),
            pltpu.VMEM((t_rows, t_cols, tile, 2 * rank_max), BF16),
            pltpu.VMEM((n_row, t_rows) + vec, F32),
            pltpu.VMEM((n_row, t_rows) + vec, F32),
            pltpu.VMEM((t_rows,) + vec, F32),
            pltpu.VMEM((t_cols, n_col) + vec, F32),
            pltpu.VMEM((t_cols,) + vec, F32),
            pltpu.VMEM((t_cols,) + vec, F32),
            pltpu.VMEM((t_rows, n_row) + vec, F32),
            pltpu.VMEM((ntile * tile // BLK, rhs_count, BLK), F32),
            dma((4 + 2 * t_rows + t_cols,)),
            dma((n_row,)),
            dma((n_row,)),
            dma((t_rows, n_row)),
            dma((t_cols, n_col)),
            dma((t_cols, n_col)),
            dma((t_rows, n_row)),
            dma((t_rows, n_row)),
            dma((ntile,)),
        ],
        compiler_params=pltpu.CompilerParams(collective_id=0, has_side_effects=True),
    )(
        root_rhs, diag_inv, tile_u[0, 0], tile_v[0, 0], tile_rank[0, 0],
        child_x, border_t, child_inv, child_blocks,
    )
    if width != share:
        me = lax.axis_index("row") * n_col + lax.axis_index("col")
        root = lax.dynamic_slice_in_dim(root, (me * share) % BLK, share, 1)
    return root, child


def solution(mesh):
    return jax.shard_map(
        per_device,
        mesh=mesh,
        in_specs=(
            P(),
            P(),
            P("row", "col", None, None, None, None),
            P("row", "col", None, None, None, None),
            P("row", "col", None, None),
            P(("row", "col"), None, None),
            P(("row", "col"), None, None),
            P(("row", "col"), None, None),
            P(("row", "col"), None),
        ),
        out_specs=(P(None, ("row", "col")), P(("row", "col"), None, None)),
        check_vma=False,
    )
```

```python
import functools
import jax
import jax.numpy as jnp
from jax import lax
from jax.experimental import pallas as pl
from jax.experimental.pallas import tpu as pltpu
from jax.sharding import PartitionSpec as P

BLK = 128
F32 = jnp.float32
BF16 = jnp.bfloat16
MESH = pl.DeviceIdType.MESH
NN = (((1,), (0,)), ((), ()))
NT = (((1,), (1,)), ((), ()))


def dot(a, b, dims=NN):
    return lax.dot_general(a, b, dims, preferred_element_type=F32)


def two_part(a):
    high = a.astype(BF16).astype(F32)
    return jnp.concatenate([high, a - high], axis=0).astype(BF16)


def wide_dot(a, b, dims=NN):
    n = a.shape[0]
    both = dot(two_part(a), b, dims)
    return both[:n] + both[n:]


def solve_kernel(
    n_row, n_col, t_rows, t_cols, ntile, n_child, bb, share,
    rhs_hbm, dinv_hbm, u_hbm, v_hbm, rank_ref, cx_ref, bt_hbm, ci_hbm, cb_ref,
    root_out, child_out,
    rhs, drow, dcol, u, v, bt, ci, w, y,
    csum, csum_in, acc, fpart, epart, xs, bacc, bpart, opart, z_all,
    out_v, out_w, out_u, out_y, in_v, in_w, in_u, in_y, pair_v, pair_w, pair_u, pair_y,
    load_sem, csend, crecv, fsend, frecv, gsend, erecv, bsend, brecv, hsend, orecv,
    xsend, xrecv, zsend, zrecv, esend, tsend, trecv, ssend, srecv,
):
    r = lax.axis_index("row")
    c = lax.axis_index("col")
    n_dev = n_row * n_col
    me = r * n_col + c
    rhs_count, tile = acc.shape[1], acc.shape[2]
    rank_max = u.shape[2]
    per = tile // BLK
    i_max = r + n_row * (t_rows - 1)

    barrier = pltpu.get_barrier_semaphore()

    def greet(o, carry):
        other = lax.rem(me + o, n_dev)
        pl.semaphore_signal(
            barrier, inc=1, device_id=(other // n_col, lax.rem(other, n_col)), device_id_type=MESH
        )
        return carry

    lax.fori_loop(1, n_dev, greet, 0)

    loads = []

    def load(src, dst):
        copy = pltpu.make_async_copy(src, dst, load_sem.at[len(loads)])
        loads.append(copy)
        copy.start()
        return copy

    bt_load = load(bt_hbm, bt)
    row_loads = [load(dinv_hbm.at[r + n_row * a], drow.at[a]) for a in range(t_rows)]
    row_loads += [
        load(rhs_hbm.at[:, pl.ds(pl.multiple_of((r + n_row * a) * tile, tile), tile)], rhs.at[a])
        for a in range(t_rows)
    ]
    u_load = load(u_hbm, u)
    v_load = load(v_hbm, v)
    col_loads = [load(dinv_hbm.at[c + n_col * b], dcol.at[b]) for b in range(t_cols)]
    ci_load = load(ci_hbm, ci)

    for b in range(t_cols):
        bacc[b] = jnp.zeros((rhs_count, tile), F32)

    def need(row, k):
        return (row + n_row * (t_rows - 1) > k) | (row == lax.rem(k, n_row))

    r_odd = lax.rem(r, 2) == 1
    c_odd = lax.rem(c, 2) == 1

    def below(i):
        return i - lax.rem(i, 2)

    def above(j):
        return j + 1 - lax.rem(j, 2)

    def need_back(row, j):
        return (row + n_row * (t_rows - 1) > above(j)) | (row == lax.rem(j, n_row))

    def fast_rows(odd):
        last = odd == ntile - 1
        first = jnp.where(last, lax.rem(odd, n_row), lax.rem(odd + 1, n_row))
        return first, lax.rem(odd + 2, n_row), jnp.logical_not(last)

    def is_fast_row(row, odd):
        first, second, both = fast_rows(odd)
        return (row == first) | (both & (row == second))

    def fast_cols(even):
        return lax.rem(even + n_col - 1, n_col), lax.rem(even + n_col - 2, n_col)

    def is_fast_col(col, even):
        first, second = fast_cols(even)
        return (col == first) | (col == second)

    for a in range(t_rows):
        i = r + n_row * a
        for rr in range(n_row):
            @pl.when(jnp.logical_not(need_back(rr, i)))
            def _():
                bpart[a, rr] = jnp.zeros((rhs_count, tile), F32)

            @pl.when(jnp.logical_not(need_back(rr, i + 1)))
            def _():
                opart[a, rr] = jnp.zeros((rhs_count, tile), F32)

    bt_load.wait()
    ups = []
    for ch in range(n_child):
        up = dot(cx_ref[ch], bt[ch])
        ups.append([up[:, m * BLK:(m + 1) * BLK] for m in range(bb)])

    def spread(j, carry):
        row = lax.rem(j, n_row)
        slot = j // n_row
        for q in range(per):
            total = jnp.zeros((rhs_count, BLK), F32)
            for ch in range(n_child):
                for m in range(bb):
                    hit = jnp.where(cb_ref[ch, m] == j * per + q, 1.0, 0.0).astype(F32)
                    total = total + ups[ch][m] * hit
            csum[row, slot, :, q * BLK:(q + 1) * BLK] = total
        return carry

    lax.fori_loop(0, ntile, spread, 0)
    pl.semaphore_wait(barrier, n_dev - 1)

    def csum_copy(rr, slot):
        return pltpu.make_async_remote_copy(
            src_ref=csum.at[rr], dst_ref=csum_in.at[slot],
            send_sem=csend.at[rr], recv_sem=crecv.at[slot],
            device_id=(rr, c), device_id_type=MESH,
        )

    def csum_start(o, carry):
        csum_copy(lax.rem(r + o, n_row), r).start()
        return carry

    lax.fori_loop(1, n_row, csum_start, 0)

    for copy in row_loads:
        copy.wait()
    u_load.wait()

    def fold_left(t, carry):
        a = t // t_cols
        b = lax.rem(t, t_cols)
        full = dot(u[a, b], drow[a])
        high = full.astype(BF16)
        w[a, b, :rank_max] = high
        w[a, b, rank_max:] = (full - high.astype(F32)).astype(BF16)
        return carry

    lax.fori_loop(0, t_rows * t_cols, fold_left, 0)
    v_load.wait()

    def owns(a):
        return r_odd & (lax.rem(r + n_row * a + n_col - 1, n_col) == c)

    def pair_copy(src, dst, send, recv, device):
        return pltpu.make_async_remote_copy(
            src_ref=src, dst_ref=dst, send_sem=send, recv_sem=recv,
            device_id=device, device_id_type=MESH,
        )

    def each_forward_pair(a, act):
        odd = r + n_row * a
        slot = odd // n_col
        col = lax.rem(odd, n_col)
        first, second, both = fast_rows(odd)

        def to(row, t):
            act(pair_copy(out_v.at[a], in_v.at[slot], tsend.at[a, t, 0], trecv.at[slot, 0], (row, col)))
            act(pair_copy(out_w.at[a], in_w.at[slot], tsend.at[a, t, 1], trecv.at[slot, 1], (row, col)))

        to(first, 0)

        @pl.when(both)
        def _():
            to(second, 1)

    def each_backward_pair(a, act):
        even = r + n_row * a - 1
        slot = even // n_row
        row = lax.rem(even, n_row)
        for t, col in enumerate(fast_cols(even)):
            act(pair_copy(out_u.at[a], in_u.at[slot], ssend.at[a, t, 0], srecv.at[slot, 0], (row, col)))
            act(pair_copy(out_y.at[a], in_y.at[slot], ssend.at[a, t, 1], srecv.at[slot, 1], (row, col)))

    def start(copy):
        copy.start()

    def send_forward_pair(a):
        @pl.when(owns(a))
        def _():
            b = (r + n_row * a - 1) // n_col
            rank = rank_ref[a, b]
            keep = lax.broadcasted_iota(jnp.int32, (tile, rank_max), 1) < rank
            out_v[a] = jnp.where(keep, v[a, b].astype(F32), 0.0)
            out_w[a] = w[a, b, :rank_max].astype(F32) + w[a, b, rank_max:].astype(F32)
            each_forward_pair(a, start)

    def send_backward_pair(a):
        @pl.when(owns(a))
        def _():
            b = (r + n_row * a - 1) // n_col
            rank = rank_ref[a, b]
            keep = lax.broadcasted_iota(jnp.int32, (rank_max, tile), 0) < rank
            out_u[a] = jnp.where(keep, u[a, b].astype(F32), 0.0)
            out_y[a] = y[a, b, :, :rank_max].astype(F32) + y[a, b, :, rank_max:].astype(F32)
            each_backward_pair(a, start)

    send_forward_pair(0)

    def csum_wait(o, carry):
        rr = lax.rem(r + o, n_row)
        csum_copy(rr, rr).wait_recv()
        return carry

    lax.fori_loop(1, n_row, csum_wait, 0)
    for a in range(t_rows):
        base = -csum[r, a]
        for o in range(1, n_row):
            base = base - csum_in[lax.rem(r + o, n_row), a]
        base = base + rhs[a].astype(F32) * jnp.where(c == 0, 1.0, 0.0).astype(F32)
        acc[a] = wide_dot(base, drow[a])

    def row_copy(a, rr, slot_b, slot_c, target_col):
        return pltpu.make_async_remote_copy(
            src_ref=acc.at[a], dst_ref=fpart.at[slot_b, slot_c],
            send_sem=fsend.at[a, rr], recv_sem=frecv.at[slot_b, slot_c],
            device_id=(rr, target_col), device_id_type=MESH,
        )

    def fast_row_copy(a, t, rr, slot_b, slot_c, target_col, odd):
        dst, sem = (fpart, frecv) if odd else (epart, erecv)
        return pltpu.make_async_remote_copy(
            src_ref=acc.at[a], dst_ref=dst.at[slot_b, slot_c],
            send_sem=gsend.at[a, t], recv_sem=sem.at[slot_b, slot_c],
            device_id=(rr, target_col), device_id_type=MESH,
        )

    def each_row_copy(a, act, own):
        i = r + n_row * a
        odd = above(i)
        odd_slot = odd // n_col
        odd_col = lax.rem(odd, n_col)
        first, second, both = fast_rows(odd)
        slot_b = i // n_col
        target = lax.rem(i, n_col)

        @pl.when(r_odd)
        def _():
            here = (first == r) & (odd_col == c)

            @pl.when(jnp.logical_not(here))
            def _():
                act(fast_row_copy(a, 0, first, odd_slot, c, odd_col, True))

            if own:
                @pl.when(here)
                def _():
                    fpart[odd_slot, c] = acc[a]

            @pl.when(both)
            def _():
                act(fast_row_copy(a, 1, second, odd_slot, c, odd_col, True))

        @pl.when(jnp.logical_not(r_odd))
        def _():
            act(fast_row_copy(a, 0, first, odd_slot, c, odd_col, False))

            @pl.when(both)
            def _():
                act(fast_row_copy(a, 1, second, odd_slot, c, odd_col, False))

            def one(t, carry):
                rr = lax.rem(r + t, n_row)

                @pl.when(need(rr, i))
                def _():
                    act(row_copy(a, rr, slot_b, c, target))

                return carry

            lax.fori_loop(1, n_row, one, 0)

            @pl.when(target != c)
            def _():
                act(row_copy(a, r, slot_b, c, target))

            if own:
                @pl.when(target == c)
                def _():
                    fpart[slot_b, c] = acc[a]

    def send_row(a):
        each_row_copy(a, start, True)

    def x_copy(b, rr):
        return pltpu.make_async_remote_copy(
            src_ref=xs.at[b], dst_ref=xs.at[b], send_sem=xsend.at[b, rr], recv_sem=xrecv.at[b],
            device_id=(rr, c), device_id_type=MESH,
        )

    def each_x_copy(b, act):
        k = c + n_col * b

        @pl.when(c_odd & (k < ntile - 1) & (r == lax.rem(k + 1, n_row)))
        def _():
            def one(t, carry):
                rr = lax.rem(r + t, n_row)

                @pl.when(need(rr, k) & jnp.logical_not(is_fast_row(rr, k)))
                def _():
                    act(x_copy(b, rr))

                return carry

            lax.fori_loop(1, n_row, one, 0)

    def col_copy(b, cc, slot_a, slot_r, target_row):
        return pltpu.make_async_remote_copy(
            src_ref=bacc.at[b], dst_ref=bpart.at[slot_a, slot_r],
            send_sem=bsend.at[b, cc], recv_sem=brecv.at[slot_a, slot_r],
            device_id=(target_row, cc), device_id_type=MESH,
        )

    def fast_col_copy(b, t, cc, slot_a, slot_r, target_row, odd):
        dst, sem = (opart, orecv) if odd else (bpart, brecv)
        return pltpu.make_async_remote_copy(
            src_ref=bacc.at[b], dst_ref=dst.at[slot_a, slot_r],
            send_sem=hsend.at[b, t], recv_sem=sem.at[slot_a, slot_r],
            device_id=(target_row, cc), device_id_type=MESH,
        )

    def each_col_copy(b, act, own):
        j = c + n_col * b
        even = below(j)
        even_slot = even // n_row
        even_row = lax.rem(even, n_row)
        slot_a = j // n_row
        target = lax.rem(j, n_row)

        @pl.when(jnp.logical_not(c_odd))
        def _():
            for t, cc in enumerate(fast_cols(even)):
                act(fast_col_copy(b, t, cc, even_slot, r, even_row, False))

        @pl.when(c_odd)
        def _():
            for t, cc in enumerate(fast_cols(even)):
                act(fast_col_copy(b, t, cc, even_slot, r, even_row, True))
            for t in range(1, n_col):
                act(col_copy(b, lax.rem(c + n_col - t, n_col), slot_a, r, target))

            @pl.when(target != r)
            def _():
                act(col_copy(b, c, slot_a, r, target))

            if own:
                @pl.when(target == r)
                def _():
                    bpart[slot_a, r] = bacc[b]

    def send_col(b):
        each_col_copy(b, start, True)

    lanes = lax.broadcasted_iota(jnp.int32, (rhs_count, rank_max), 1)

    def live(value, a, b):
        kept = jnp.where(lanes < rank_ref[a, b], value, 0.0).astype(BF16)
        return jnp.concatenate([kept, kept], axis=1)

    for a in range(t_rows):
        @pl.when(below(r + n_row * a) <= c)
        def _():
            send_row(a)

    for copy in col_loads:
        copy.wait()

    def forward(b, carry):
        k = c + n_col * b
        k_row = lax.rem(k, n_row)

        @pl.when(need(r, k))
        def _():
            fast = is_fast_row(r, k)

            @pl.when(jnp.logical_not(c_odd))
            def _():
                for cc in range(n_col):
                    @pl.when(jnp.logical_not((r == k_row) & (c == cc)))
                    def _():
                        row_copy(0, lax.rem(r + 1, n_row), b, cc, c).wait_recv()

                x = fpart[b, 0]
                for cc in range(1, n_col):
                    x = x + fpart[b, cc]
                xs[b] = x

            @pl.when(c_odd & jnp.logical_not(fast))
            def _():
                x_copy(b, lax.rem(r + 1, n_row)).wait_recv()

            @pl.when(c_odd & fast)
            def _():
                away = (lax.rem(r + 1, n_row), c)
                pair_copy(out_v.at[0], in_v.at[b], tsend.at[0, 0, 0], trecv.at[b, 0], away).wait_recv()
                pair_copy(out_w.at[0], in_w.at[b], tsend.at[0, 0, 1], trecv.at[b, 1], away).wait_recv()
                pair_v[...] = in_v[b].astype(BF16)
                full = in_w[b]
                high = full.astype(BF16)
                pair_w[:rank_max] = high
                pair_w[rank_max:] = (full - high.astype(F32)).astype(BF16)
                for cc in range(n_col):
                    fast_row_copy(0, 0, lax.rem(r + 1, n_row), b, cc, c, False).wait_recv()
                x = epart[b, 0]
                for cc in range(1, n_col):
                    x = x + epart[b, cc]
                p = dot(x.astype(BF16), pair_v[...]).astype(BF16)
                part = dot(jnp.concatenate([p, p], axis=1), pair_w[...])
                for cc in range(n_col):
                    @pl.when(jnp.logical_not((r == k_row) & (c == cc)))
                    def _():
                        row_copy(0, lax.rem(r + 1, n_row), b, cc, c).wait_recv()

                x = fpart[b, 0]
                for cc in range(1, n_col):
                    x = x + fpart[b, cc]
                xs[b] = x - part

            x = xs[b]
            xb = x.astype(BF16)
            for a in range(t_rows):
                i = r + n_row * a

                @pl.when(below(i) > k)
                def _():
                    p = live(dot(xb, v[a, b]), a, b)
                    acc[a] = acc[a] - dot(p, w[a, b])

                    @pl.when(below(i) <= k + n_col)
                    def _():
                        send_row(a)

            each_x_copy(b, start)

            @pl.when(r == k_row)
            def _():
                bacc[b] = wide_dot(xs[b], drow[k // n_row], NT)

                @pl.when(above(k) >= i_max)
                def _():
                    send_col(b)

        @pl.when(b == 0)
        def _():
            def fold_right(t, inner):
                a = t // t_cols
                bq = lax.rem(t, t_cols)
                full = dot(dcol[bq], v[a, bq])
                high = full.astype(BF16)
                y[a, bq, :, :rank_max] = high
                y[a, bq, :, rank_max:] = (full - high.astype(F32)).astype(BF16)
                return inner

            lax.fori_loop(0, t_rows * t_cols, fold_right, 0)
            for a in range(1, t_rows):
                send_forward_pair(a)
            if t_cols == 1:
                for a in reversed(range(t_rows)):
                    send_backward_pair(a)

        if t_cols > 1:
            @pl.when(b == 1)
            def _():
                for a in reversed(range(t_rows)):
                    send_backward_pair(a)

        return carry

    lax.fori_loop(0, t_cols, forward, 0)

    def z_copy(a, rr, i):
        part = z_all.at[pl.ds(i * per, per)]
        return pltpu.make_async_remote_copy(
            src_ref=part, dst_ref=part, send_sem=zsend.at[a, rr], recv_sem=zrecv.at[i],
            device_id=(rr, c), device_id_type=MESH,
        )

    def z_even_copy(a, cc, i):
        part = z_all.at[pl.ds(i * per, per)]
        return pltpu.make_async_remote_copy(
            src_ref=part, dst_ref=part, send_sem=esend.at[a, cc], recv_sem=zrecv.at[i],
            device_id=(r, cc), device_id_type=MESH,
        )

    def each_z_even(a, act):
        i = r + n_row * a

        @pl.when(jnp.logical_not(r_odd) & (c == fast_cols(i)[0]))
        def _():
            for t in range(1, n_col):
                cc = lax.rem(c + t, n_col)

                @pl.when(jnp.logical_not(is_fast_col(cc, i)))
                def _():
                    act(z_even_copy(a, cc, i))

    for a in reversed(range(t_rows)):
        i = r + n_row * a
        i_col = lax.rem(i, n_col)

        def wait_part(rr, carry):
            @pl.when(need_back(rr, i) & jnp.logical_not((rr == r) & (c == i_col)))
            def _():
                col_copy(0, lax.rem(c + 1, n_col), a, rr, r).wait_recv()

            return carry

        def put(z):
            for q in range(per):
                z_all[i * per + q] = z[:, q * BLK:(q + 1) * BLK]

        fast = is_fast_col(c, i)

        @pl.when(r_odd)
        def _():
            lax.fori_loop(0, n_row, wait_part, 0)
            z = bpart[a, 0]
            for rr in range(1, n_row):
                z = z + bpart[a, rr]
            put(z)

        @pl.when(jnp.logical_not(r_odd | fast))
        def _():
            z_even_copy(a, lax.rem(c + 1, n_col), i).wait_recv()

        @pl.when(jnp.logical_not(r_odd) & fast)
        def _():
            away = (r, lax.rem(c + 1, n_col))
            pair_copy(out_u.at[0], in_u.at[a], ssend.at[0, 0, 0], srecv.at[a, 0], away).wait_recv()
            pair_copy(out_y.at[0], in_y.at[a], ssend.at[0, 0, 1], srecv.at[a, 1], away).wait_recv()
            pair_u[...] = in_u[a].astype(BF16)
            full = in_y[a]
            high = full.astype(BF16)
            pair_y[:, :rank_max] = high
            pair_y[:, rank_max:] = (full - high.astype(F32)).astype(BF16)

            def wait_odd(rr, carry):
                @pl.when(need_back(rr, i + 1))
                def _():
                    fast_col_copy(0, 0, lax.rem(c + 1, n_col), a, rr, r, True).wait_recv()

                return carry

            lax.fori_loop(0, n_row, wait_odd, 0)
            z = opart[a, 0]
            for rr in range(1, n_row):
                z = z + opart[a, rr]
            p = dot(z.astype(BF16), pair_u[...], NT).astype(BF16)
            part = dot(jnp.concatenate([p, p], axis=1), pair_y[...], NT)
            lax.fori_loop(0, n_row, wait_part, 0)
            z = bpart[a, 0]
            for rr in range(1, n_row):
                z = z + bpart[a, rr]
            put(z - part)

        z = jnp.concatenate([z_all[i * per + q] for q in range(per)], axis=1)
        zb = z.astype(BF16)

        def back(t, carry):
            b = t_cols - 1 - t
            j = c + n_col * b

            @pl.when(above(j) < i)
            def _():
                q = live(dot(zb, u[a, b], NT), a, b)
                bacc[b] = bacc[b] - dot(q, y[a, b], NT)

                @pl.when(above(j) >= i - n_row)
                def _():
                    send_col(b)

            return carry

        lax.fori_loop(0, t_cols, back, 0)
        each_z_even(a, start)

        def z_start(o, carry):
            z_copy(a, lax.rem(r + o, n_row), i).start()
            return carry

        lax.fori_loop(1, n_row, z_start, 0)

    def z_wait(j, carry):
        @pl.when(lax.rem(j, n_row) != r)
        def _():
            z_copy(0, lax.rem(r + 1, n_row), j).wait_recv()

        return carry

    lax.fori_loop(0, ntile, z_wait, 0)

    if share % BLK == 0:
        for q in range(share // BLK):
            root_out[:, q * BLK:(q + 1) * BLK] = z_all[me * (share // BLK) + q]
    else:
        first = (me * share) // BLK
        root_out[...] = z_all[first]
    ci_load.wait()
    for ch in range(n_child):
        taken = jnp.concatenate([z_all[cb_ref[ch, m]] for m in range(bb)], axis=1).astype(BF16)
        returned = dot(taken, bt[ch], NT)
        child_out[ch] = cx_ref[ch].astype(F32) - wide_dot(returned, ci[ch])

    def sent(copy):
        copy.wait_send()

    def csum_done(o, carry):
        csum_copy(lax.rem(r + o, n_row), r).wait_send()
        return carry

    lax.fori_loop(1, n_row, csum_done, 0)
    for a in range(t_rows):
        each_row_copy(a, sent, False)
        each_z_even(a, sent)

        @pl.when(owns(a))
        def _():
            each_forward_pair(a, sent)
            each_backward_pair(a, sent)

        def z_done(o, carry):
            z_copy(a, lax.rem(r + o, n_row), r + n_row * a).wait_send()
            return carry

        lax.fori_loop(1, n_row, z_done, 0)
    for b in range(t_cols):
        @pl.when(need_back(r, c + n_col * b))
        def _():
            each_col_copy(b, sent, False)

        each_x_copy(b, sent)


def per_device(
    root_rhs, diag_inv, tile_u, tile_v, tile_rank, child_x, border_t, child_inv, child_blocks
):
    n_row = lax.axis_size("row")
    n_col = lax.axis_size("col")
    ntile, tile = diag_inv.shape[0], diag_inv.shape[1]
    rhs_count = root_rhs.shape[0]
    t_rows, t_cols, rank_max = tile_u.shape[2], tile_u.shape[3], tile_u.shape[4]
    n_child, bb = child_blocks.shape
    share = ntile * tile // (n_row * n_col)
    width = share if share % BLK == 0 else BLK
    vec = (rhs_count, tile)
    any_spec = pl.BlockSpec(memory_space=pl.ANY)
    vmem = pl.BlockSpec(memory_space=pltpu.VMEM)
    smem = pl.BlockSpec(memory_space=pltpu.SMEM)
    dma = pltpu.SemaphoreType.DMA
    root, child = pl.pallas_call(
        functools.partial(
            solve_kernel, n_row, n_col, t_rows, t_cols, ntile, n_child, bb, share
        ),
        out_shape=(
            jax.ShapeDtypeStruct((rhs_count, width), F32),
            jax.ShapeDtypeStruct(child_x.shape, F32),
        ),
        in_specs=[any_spec, any_spec, any_spec, any_spec, smem, vmem, any_spec, any_spec, smem],
        out_specs=(vmem, vmem),
        scratch_shapes=[
            pltpu.VMEM((t_rows,) + vec, BF16),
            pltpu.VMEM((t_rows, tile, tile), BF16),
            pltpu.VMEM((t_cols, tile, tile), BF16),
            pltpu.VMEM(tile_u.shape[2:], BF16),
            pltpu.VMEM(tile_v.shape[2:], BF16),
            pltpu.VMEM(border_t.shape, BF16),
            pltpu.VMEM(child_inv.shape, BF16),
            pltpu.VMEM((t_rows, t_cols, 2 * rank_max, tile), BF16),
            pltpu.VMEM((t_rows, t_cols, tile, 2 * rank_max), BF16),
            pltpu.VMEM((n_row, t_rows) + vec, F32),
            pltpu.VMEM((n_row, t_rows) + vec, F32),
            pltpu.VMEM((t_rows,) + vec, F32),
            pltpu.VMEM((t_cols, n_col) + vec, F32),
            pltpu.VMEM((t_cols, n_col) + vec, F32),
            pltpu.VMEM((t_cols,) + vec, F32),
            pltpu.VMEM((t_cols,) + vec, F32),
            pltpu.VMEM((t_rows, n_row) + vec, F32),
            pltpu.VMEM((t_rows, n_row) + vec, F32),
            pltpu.VMEM((ntile * tile // BLK, rhs_count, BLK), F32),
            pltpu.VMEM((t_rows, tile, rank_max), F32),
            pltpu.VMEM((t_rows, rank_max, tile), F32),
            pltpu.VMEM((t_rows, rank_max, tile), F32),
            pltpu.VMEM((t_rows, tile, rank_max), F32),
            pltpu.VMEM((t_cols, tile, rank_max), F32),
            pltpu.VMEM((t_cols, rank_max, tile), F32),
            pltpu.VMEM((t_rows, rank_max, tile), F32),
            pltpu.VMEM((t_rows, tile, rank_max), F32),
            pltpu.VMEM((tile, rank_max), BF16),
            pltpu.VMEM((2 * rank_max, tile), BF16),
            pltpu.VMEM((rank_max, tile), BF16),
            pltpu.VMEM((tile, 2 * rank_max), BF16),
            dma((4 + 2 * t_rows + t_cols,)),
            dma((n_row,)),
            dma((n_row,)),
            dma((t_rows, n_row)),
            dma((t_cols, n_col)),
            dma((t_rows, 2)),
            dma((t_cols, n_col)),
            dma((t_cols, n_col)),
            dma((t_rows, n_row)),
            dma((t_cols, 2)),
            dma((t_rows, n_row)),
            dma((t_cols, n_row)),
            dma((t_cols,)),
            dma((t_rows, n_row)),
            dma((ntile,)),
            dma((t_rows, n_col)),
            dma((t_rows, 2, 2)),
            dma((t_cols, 2)),
            dma((t_rows, 2, 2)),
            dma((t_rows, 2)),
        ],
        compiler_params=pltpu.CompilerParams(collective_id=0, has_side_effects=True),
    )(
        root_rhs, diag_inv, tile_u[0, 0], tile_v[0, 0], tile_rank[0, 0],
        child_x, border_t, child_inv, child_blocks,
    )
    if width != share:
        me = lax.axis_index("row") * n_col + lax.axis_index("col")
        root = lax.dynamic_slice_in_dim(root, (me * share) % BLK, share, 1)
    return root, child


def solution(mesh):
    return jax.shard_map(
        per_device,
        mesh=mesh,
        in_specs=(
            P(),
            P(),
            P("row", "col", None, None, None, None),
            P("row", "col", None, None, None, None),
            P("row", "col", None, None),
            P(("row", "col"), None, None),
            P(("row", "col"), None, None),
            P(("row", "col"), None, None),
            P(("row", "col"), None),
        ),
        out_specs=(P(None, ("row", "col")), P(("row", "col"), None, None)),
        check_vma=False,
    )
```

```python
import functools
import jax
import jax.numpy as jnp
from jax import lax
from jax.experimental import pallas as pl
from jax.experimental.pallas import tpu as pltpu
from jax.sharding import PartitionSpec as P

BLK = 128
F32 = jnp.float32
BF16 = jnp.bfloat16
MESH = pl.DeviceIdType.MESH
NN = (((1,), (0,)), ((), ()))
NT = (((1,), (1,)), ((), ()))


def dot(a, b, dims=NN):
    return lax.dot_general(a, b, dims, preferred_element_type=F32)


def two_part(a):
    high = a.astype(BF16).astype(F32)
    return jnp.concatenate([high, a - high], axis=0).astype(BF16)


def wide_dot(a, b, dims=NN):
    n = a.shape[0]
    both = dot(two_part(a), b, dims)
    return both[:n] + both[n:]


def solve_kernel(
    n_row, n_col, t_rows, t_cols, ntile, n_child, bb, share,
    rhs_hbm, dinv_hbm, u_hbm, v_hbm, rank_ref, cx_ref, bt_hbm, ci_hbm, cb_ref,
    root_out, child_out,
    rhs, drow, dcol, u, v, bt, ci, w, y,
    csum, csum_in, acc, fpart, epart, xs, bacc, bpart, opart, z_all,
    out_v, out_w, out_u, out_y, in_v, in_w, in_u, in_y, pair_v, pair_w, pair_u, pair_y,
    load_sem, csend, crecv, fsend, frecv, gsend, erecv, bsend, brecv, hsend, orecv,
    xsend, xrecv, zsend, zrecv, esend, tsend, trecv, ssend, srecv,
):
    r = lax.axis_index("row")
    c = lax.axis_index("col")
    n_dev = n_row * n_col
    me = r * n_col + c
    rhs_count, tile = acc.shape[1], acc.shape[2]
    rank_max = u.shape[2]
    per = tile // BLK
    i_max = r + n_row * (t_rows - 1)

    barrier = pltpu.get_barrier_semaphore()

    def greet(o, carry):
        other = lax.rem(me + o, n_dev)
        pl.semaphore_signal(
            barrier, inc=1, device_id=(other // n_col, lax.rem(other, n_col)), device_id_type=MESH
        )
        return carry

    lax.fori_loop(1, n_dev, greet, 0)

    loads = []

    def load(src, dst):
        copy = pltpu.make_async_copy(src, dst, load_sem.at[len(loads)])
        loads.append(copy)
        copy.start()
        return copy

    bt_load = load(bt_hbm, bt)
    row_loads = [load(dinv_hbm.at[r + n_row * a], drow.at[a]) for a in range(t_rows)]
    row_loads += [
        load(rhs_hbm.at[:, pl.ds(pl.multiple_of((r + n_row * a) * tile, tile), tile)], rhs.at[a])
        for a in range(t_rows)
    ]
    u_load = load(u_hbm, u)
    v_load = load(v_hbm, v)
    col_loads = [load(dinv_hbm.at[c + n_col * b], dcol.at[b]) for b in range(t_cols)]
    ci_load = load(ci_hbm, ci)

    for b in range(t_cols):
        bacc[b] = jnp.zeros((rhs_count, tile), F32)

    def need(row, k):
        return (row + n_row * (t_rows - 1) > k) | (row == lax.rem(k, n_row))

    r_odd = lax.rem(r, 2) == 1
    c_odd = lax.rem(c, 2) == 1

    def below(i):
        return i - lax.rem(i, 2)

    def above(j):
        return j + 1 - lax.rem(j, 2)

    def need_back(row, j):
        return (row + n_row * (t_rows - 1) > above(j)) | (row == lax.rem(j, n_row))

    def fast_rows(odd):
        last = odd == ntile - 1
        first = jnp.where(last, lax.rem(odd, n_row), lax.rem(odd + 1, n_row))
        return first, lax.rem(odd + 2, n_row), jnp.logical_not(last)

    def is_fast_row(row, odd):
        first, second, both = fast_rows(odd)
        return (row == first) | (both & (row == second))

    def fast_cols(even):
        return (lax.rem(even + n_col - 1, n_col),)

    def is_fast_col(col, even):
        return col == fast_cols(even)[0]

    for a in range(t_rows):
        i = r + n_row * a
        for rr in range(n_row):
            @pl.when(jnp.logical_not(need_back(rr, i)))
            def _():
                bpart[a, rr] = jnp.zeros((rhs_count, tile), F32)

            @pl.when(jnp.logical_not(need_back(rr, i + 1)))
            def _():
                opart[a, rr] = jnp.zeros((rhs_count, tile), F32)

    bt_load.wait()
    ups = []
    for ch in range(n_child):
        up = dot(cx_ref[ch], bt[ch])
        ups.append([up[:, m * BLK:(m + 1) * BLK] for m in range(bb)])

    def spread(j, carry):
        row = lax.rem(j, n_row)
        slot = j // n_row
        for q in range(per):
            total = jnp.zeros((rhs_count, BLK), F32)
            for ch in range(n_child):
                for m in range(bb):
                    hit = jnp.where(cb_ref[ch, m] == j * per + q, 1.0, 0.0).astype(F32)
                    total = total + ups[ch][m] * hit
            csum[row, slot, :, q * BLK:(q + 1) * BLK] = total
        return carry

    lax.fori_loop(0, ntile, spread, 0)
    pl.semaphore_wait(barrier, n_dev - 1)

    def csum_copy(rr, slot):
        return pltpu.make_async_remote_copy(
            src_ref=csum.at[rr], dst_ref=csum_in.at[slot],
            send_sem=csend.at[rr], recv_sem=crecv.at[slot],
            device_id=(rr, c), device_id_type=MESH,
        )

    def csum_start(o, carry):
        csum_copy(lax.rem(r + o, n_row), r).start()
        return carry

    lax.fori_loop(1, n_row, csum_start, 0)

    for copy in row_loads:
        copy.wait()
    u_load.wait()
    v_load.wait()

    def fold_left(t, carry):
        a = t // t_cols
        b = lax.rem(t, t_cols)
        full = dot(u[a, b], drow[a])
        high = full.astype(BF16)
        w[a, b, :rank_max] = high
        w[a, b, rank_max:] = (full - high.astype(F32)).astype(BF16)
        return carry


    def owns(a):
        return r_odd & (lax.rem(r + n_row * a + n_col - 1, n_col) == c)

    def pair_copy(src, dst, send, recv, device):
        return pltpu.make_async_remote_copy(
            src_ref=src, dst_ref=dst, send_sem=send, recv_sem=recv,
            device_id=device, device_id_type=MESH,
        )

    def each_forward_pair(a, act):
        odd = r + n_row * a
        slot = odd // n_col
        col = lax.rem(odd, n_col)
        first, second, both = fast_rows(odd)

        def to(row, t):
            act(pair_copy(out_v.at[a], in_v.at[slot], tsend.at[a, t, 0], trecv.at[slot, 0], (row, col)))
            act(pair_copy(out_w.at[a], in_w.at[slot], tsend.at[a, t, 1], trecv.at[slot, 1], (row, col)))

        to(first, 0)

        @pl.when(both)
        def _():
            to(second, 1)

    def each_backward_pair(a, act):
        even = r + n_row * a - 1
        slot = even // n_row
        row = lax.rem(even, n_row)
        for t, col in enumerate(fast_cols(even)):
            act(pair_copy(out_u.at[a], in_u.at[slot], ssend.at[a, t, 0], srecv.at[slot, 0], (row, col)))
            act(pair_copy(out_y.at[a], in_y.at[slot], ssend.at[a, t, 1], srecv.at[slot, 1], (row, col)))

    def start(copy):
        copy.start()

    def send_forward_pair(a):
        @pl.when(owns(a))
        def _():
            b = (r + n_row * a - 1) // n_col
            rank = rank_ref[a, b]
            keep = lax.broadcasted_iota(jnp.int32, (tile, rank_max), 1) < rank
            out_v[a] = jnp.where(keep, v[a, b].astype(F32), 0.0)
            out_w[a] = dot(u[a, b], drow[a])
            each_forward_pair(a, start)

    def send_backward_pair(a):
        @pl.when(owns(a))
        def _():
            b = (r + n_row * a - 1) // n_col
            rank = rank_ref[a, b]
            keep = lax.broadcasted_iota(jnp.int32, (rank_max, tile), 0) < rank
            out_u[a] = jnp.where(keep, u[a, b].astype(F32), 0.0)
            out_y[a] = y[a, b, :, :rank_max].astype(F32) + y[a, b, :, rank_max:].astype(F32)
            each_backward_pair(a, start)

    send_forward_pair(0)
    lax.fori_loop(0, t_rows * t_cols, fold_left, 0)

    def csum_wait(o, carry):
        rr = lax.rem(r + o, n_row)
        csum_copy(rr, rr).wait_recv()
        return carry

    lax.fori_loop(1, n_row, csum_wait, 0)
    for a in range(t_rows):
        base = -csum[r, a]
        for o in range(1, n_row):
            base = base - csum_in[lax.rem(r + o, n_row), a]
        base = base + rhs[a].astype(F32) * jnp.where(c == 0, 1.0, 0.0).astype(F32)
        acc[a] = wide_dot(base, drow[a])

    def row_copy(a, rr, slot_b, slot_c, target_col):
        return pltpu.make_async_remote_copy(
            src_ref=acc.at[a], dst_ref=fpart.at[slot_b, slot_c],
            send_sem=fsend.at[a, rr], recv_sem=frecv.at[slot_b, slot_c],
            device_id=(rr, target_col), device_id_type=MESH,
        )

    def fast_row_copy(a, t, rr, slot_b, slot_c, target_col, odd):
        dst, sem = (fpart, frecv) if odd else (epart, erecv)
        return pltpu.make_async_remote_copy(
            src_ref=acc.at[a], dst_ref=dst.at[slot_b, slot_c],
            send_sem=gsend.at[a, t], recv_sem=sem.at[slot_b, slot_c],
            device_id=(rr, target_col), device_id_type=MESH,
        )

    def each_row_copy(a, act, own):
        i = r + n_row * a
        odd = above(i)
        odd_slot = odd // n_col
        odd_col = lax.rem(odd, n_col)
        first, second, both = fast_rows(odd)
        slot_b = i // n_col
        target = lax.rem(i, n_col)

        @pl.when(r_odd)
        def _():
            here = (first == r) & (odd_col == c)

            @pl.when(jnp.logical_not(here))
            def _():
                act(fast_row_copy(a, 0, first, odd_slot, c, odd_col, True))

            if own:
                @pl.when(here)
                def _():
                    fpart[odd_slot, c] = acc[a]

            @pl.when(both)
            def _():
                act(fast_row_copy(a, 1, second, odd_slot, c, odd_col, True))

        @pl.when(jnp.logical_not(r_odd))
        def _():
            act(fast_row_copy(a, 0, first, odd_slot, c, odd_col, False))

            @pl.when(both)
            def _():
                act(fast_row_copy(a, 1, second, odd_slot, c, odd_col, False))

            def one(t, carry):
                rr = lax.rem(r + t, n_row)

                @pl.when(need(rr, i))
                def _():
                    act(row_copy(a, rr, slot_b, c, target))

                return carry

            lax.fori_loop(1, n_row, one, 0)

            @pl.when(target != c)
            def _():
                act(row_copy(a, r, slot_b, c, target))

            if own:
                @pl.when(target == c)
                def _():
                    fpart[slot_b, c] = acc[a]

    def send_row(a):
        each_row_copy(a, start, True)

    def x_copy(b, rr):
        return pltpu.make_async_remote_copy(
            src_ref=xs.at[b], dst_ref=xs.at[b], send_sem=xsend.at[b, rr], recv_sem=xrecv.at[b],
            device_id=(rr, c), device_id_type=MESH,
        )

    def each_x_copy(b, act):
        k = c + n_col * b

        @pl.when(c_odd & (k < ntile - 1) & (r == lax.rem(k + 1, n_row)))
        def _():
            def one(t, carry):
                rr = lax.rem(r + t, n_row)

                @pl.when(need(rr, k) & jnp.logical_not(is_fast_row(rr, k)))
                def _():
                    act(x_copy(b, rr))

                return carry

            lax.fori_loop(1, n_row, one, 0)

    def col_copy(b, cc, slot_a, slot_r, target_row):
        return pltpu.make_async_remote_copy(
            src_ref=bacc.at[b], dst_ref=bpart.at[slot_a, slot_r],
            send_sem=bsend.at[b, cc], recv_sem=brecv.at[slot_a, slot_r],
            device_id=(target_row, cc), device_id_type=MESH,
        )

    def fast_col_copy(b, t, cc, slot_a, slot_r, target_row, odd):
        dst, sem = (opart, orecv) if odd else (bpart, brecv)
        return pltpu.make_async_remote_copy(
            src_ref=bacc.at[b], dst_ref=dst.at[slot_a, slot_r],
            send_sem=hsend.at[b, t], recv_sem=sem.at[slot_a, slot_r],
            device_id=(target_row, cc), device_id_type=MESH,
        )

    def each_col_copy(b, act, own):
        j = c + n_col * b
        even = below(j)
        even_slot = even // n_row
        even_row = lax.rem(even, n_row)
        slot_a = j // n_row
        target = lax.rem(j, n_row)

        @pl.when(jnp.logical_not(c_odd))
        def _():
            for t, cc in enumerate(fast_cols(even)):
                act(fast_col_copy(b, t, cc, even_slot, r, even_row, False))

        @pl.when(c_odd)
        def _():
            for t, cc in enumerate(fast_cols(even)):
                act(fast_col_copy(b, t, cc, even_slot, r, even_row, True))
            for t in range(1, n_col):
                act(col_copy(b, lax.rem(c + n_col - t, n_col), slot_a, r, target))

            @pl.when(target != r)
            def _():
                act(col_copy(b, c, slot_a, r, target))

            if own:
                @pl.when(target == r)
                def _():
                    bpart[slot_a, r] = bacc[b]

    def send_col(b):
        each_col_copy(b, start, True)

    lanes = lax.broadcasted_iota(jnp.int32, (rhs_count, rank_max), 1)

    def live(value, a, b):
        kept = jnp.where(lanes < rank_ref[a, b], value, 0.0).astype(BF16)
        return jnp.concatenate([kept, kept], axis=1)

    for a in range(t_rows):
        @pl.when(below(r + n_row * a) <= c)
        def _():
            send_row(a)

    for copy in col_loads:
        copy.wait()

    def forward(b, carry):
        k = c + n_col * b
        k_row = lax.rem(k, n_row)

        @pl.when(need(r, k))
        def _():
            fast = is_fast_row(r, k)

            @pl.when(jnp.logical_not(c_odd))
            def _():
                for cc in range(n_col):
                    @pl.when(jnp.logical_not((r == k_row) & (c == cc)))
                    def _():
                        row_copy(0, lax.rem(r + 1, n_row), b, cc, c).wait_recv()

                x = fpart[b, 0]
                for cc in range(1, n_col):
                    x = x + fpart[b, cc]
                xs[b] = x

            @pl.when(c_odd & jnp.logical_not(fast))
            def _():
                x_copy(b, lax.rem(r + 1, n_row)).wait_recv()

            @pl.when(c_odd & fast)
            def _():
                away = (lax.rem(r + 1, n_row), c)
                pair_copy(out_v.at[0], in_v.at[b], tsend.at[0, 0, 0], trecv.at[b, 0], away).wait_recv()
                pair_copy(out_w.at[0], in_w.at[b], tsend.at[0, 0, 1], trecv.at[b, 1], away).wait_recv()
                pair_v[...] = in_v[b].astype(BF16)
                full = in_w[b]
                high = full.astype(BF16)
                pair_w[:rank_max] = high
                pair_w[rank_max:] = (full - high.astype(F32)).astype(BF16)
                for cc in range(n_col):
                    fast_row_copy(0, 0, lax.rem(r + 1, n_row), b, cc, c, False).wait_recv()
                x = epart[b, 0]
                for cc in range(1, n_col):
                    x = x + epart[b, cc]
                p = dot(x.astype(BF16), pair_v[...]).astype(BF16)
                part = dot(jnp.concatenate([p, p], axis=1), pair_w[...])
                for cc in range(n_col):
                    @pl.when(jnp.logical_not((r == k_row) & (c == cc)))
                    def _():
                        row_copy(0, lax.rem(r + 1, n_row), b, cc, c).wait_recv()

                x = fpart[b, 0]
                for cc in range(1, n_col):
                    x = x + fpart[b, cc]
                xs[b] = x - part

            x = xs[b]
            xb = x.astype(BF16)
            for a in range(t_rows):
                i = r + n_row * a

                @pl.when(below(i) > k)
                def _():
                    p = live(dot(xb, v[a, b]), a, b)
                    acc[a] = acc[a] - dot(p, w[a, b])

                    @pl.when(below(i) <= k + n_col)
                    def _():
                        send_row(a)

            each_x_copy(b, start)

            @pl.when(r == k_row)
            def _():
                bacc[b] = wide_dot(xs[b], drow[k // n_row], NT)

                @pl.when(above(k) >= i_max)
                def _():
                    send_col(b)

        @pl.when(b == 0)
        def _():
            def fold_right(t, inner):
                a = t // t_cols
                bq = lax.rem(t, t_cols)
                full = dot(dcol[bq], v[a, bq])
                high = full.astype(BF16)
                y[a, bq, :, :rank_max] = high
                y[a, bq, :, rank_max:] = (full - high.astype(F32)).astype(BF16)
                return inner

            lax.fori_loop(0, t_rows * t_cols, fold_right, 0)
            for a in range(1, t_rows):
                send_forward_pair(a)
            if t_cols == 1:
                for a in reversed(range(t_rows)):
                    send_backward_pair(a)

        if t_cols > 1:
            for step, a in enumerate(reversed(range(t_rows))):
                @pl.when(b == min(1 + step, t_cols - 1))
                def _():
                    send_backward_pair(a)

        return carry

    lax.fori_loop(0, t_cols, forward, 0)

    def z_copy(a, rr, i):
        part = z_all.at[pl.ds(i * per, per)]
        return pltpu.make_async_remote_copy(
            src_ref=part, dst_ref=part, send_sem=zsend.at[a, rr], recv_sem=zrecv.at[i],
            device_id=(rr, c), device_id_type=MESH,
        )

    def z_even_copy(a, cc, i):
        part = z_all.at[pl.ds(i * per, per)]
        return pltpu.make_async_remote_copy(
            src_ref=part, dst_ref=part, send_sem=esend.at[a, cc], recv_sem=zrecv.at[i],
            device_id=(r, cc), device_id_type=MESH,
        )

    def each_z_even(a, act):
        i = r + n_row * a

        @pl.when(jnp.logical_not(r_odd) & (c == fast_cols(i)[0]))
        def _():
            for t in range(1, n_col):
                act(z_even_copy(a, lax.rem(c + n_col - t, n_col), i))

    for a in reversed(range(t_rows)):
        i = r + n_row * a
        i_col = lax.rem(i, n_col)

        def wait_part(rr, carry):
            @pl.when(need_back(rr, i) & jnp.logical_not((rr == r) & (c == i_col)))
            def _():
                col_copy(0, lax.rem(c + 1, n_col), a, rr, r).wait_recv()

            return carry

        def put(z):
            for q in range(per):
                z_all[i * per + q] = z[:, q * BLK:(q + 1) * BLK]

        fast = is_fast_col(c, i)

        @pl.when(r_odd)
        def _():
            lax.fori_loop(0, n_row, wait_part, 0)
            z = bpart[a, 0]
            for rr in range(1, n_row):
                z = z + bpart[a, rr]
            put(z)

        @pl.when(jnp.logical_not(r_odd | fast))
        def _():
            z_even_copy(a, lax.rem(c + 1, n_col), i).wait_recv()

        @pl.when(jnp.logical_not(r_odd) & fast)
        def _():
            away = (r, lax.rem(c + 1, n_col))
            pair_copy(out_u.at[0], in_u.at[a], ssend.at[0, 0, 0], srecv.at[a, 0], away).wait_recv()
            pair_copy(out_y.at[0], in_y.at[a], ssend.at[0, 0, 1], srecv.at[a, 1], away).wait_recv()
            pair_u[...] = in_u[a].astype(BF16)
            full = in_y[a]
            high = full.astype(BF16)
            pair_y[:, :rank_max] = high
            pair_y[:, rank_max:] = (full - high.astype(F32)).astype(BF16)

            def wait_odd(rr, carry):
                @pl.when(need_back(rr, i + 1))
                def _():
                    fast_col_copy(0, 0, lax.rem(c + 1, n_col), a, rr, r, True).wait_recv()

                return carry

            lax.fori_loop(0, n_row, wait_odd, 0)
            z = opart[a, 0]
            for rr in range(1, n_row):
                z = z + opart[a, rr]
            p = dot(z.astype(BF16), pair_u[...], NT).astype(BF16)
            part = dot(jnp.concatenate([p, p], axis=1), pair_y[...], NT)
            lax.fori_loop(0, n_row, wait_part, 0)
            z = bpart[a, 0]
            for rr in range(1, n_row):
                z = z + bpart[a, rr]
            put(z - part)

        z = jnp.concatenate([z_all[i * per + q] for q in range(per)], axis=1)
        each_z_even(a, start)
        zb = z.astype(BF16)

        def back(t, carry):
            b = t_cols - 1 - t
            j = c + n_col * b

            @pl.when(above(j) < i)
            def _():
                q = live(dot(zb, u[a, b], NT), a, b)
                bacc[b] = bacc[b] - dot(q, y[a, b], NT)

                @pl.when(above(j) >= i - n_row)
                def _():
                    send_col(b)

            return carry

        lax.fori_loop(0, t_cols, back, 0)

        def z_start(o, carry):
            z_copy(a, lax.rem(r + o, n_row), i).start()
            return carry

        lax.fori_loop(1, n_row, z_start, 0)

    def z_wait(j, carry):
        @pl.when(lax.rem(j, n_row) != r)
        def _():
            z_copy(0, lax.rem(r + 1, n_row), j).wait_recv()

        return carry

    lax.fori_loop(0, ntile, z_wait, 0)

    if share % BLK == 0:
        for q in range(share // BLK):
            root_out[:, q * BLK:(q + 1) * BLK] = z_all[me * (share // BLK) + q]
    else:
        first = (me * share) // BLK
        root_out[...] = z_all[first]
    ci_load.wait()
    for ch in range(n_child):
        taken = jnp.concatenate([z_all[cb_ref[ch, m]] for m in range(bb)], axis=1).astype(BF16)
        returned = dot(taken, bt[ch], NT)
        child_out[ch] = cx_ref[ch].astype(F32) - wide_dot(returned, ci[ch])

    def sent(copy):
        copy.wait_send()

    def csum_done(o, carry):
        csum_copy(lax.rem(r + o, n_row), r).wait_send()
        return carry

    lax.fori_loop(1, n_row, csum_done, 0)
    for a in range(t_rows):
        each_row_copy(a, sent, False)
        each_z_even(a, sent)

        @pl.when(owns(a))
        def _():
            each_forward_pair(a, sent)
            each_backward_pair(a, sent)

        def z_done(o, carry):
            z_copy(a, lax.rem(r + o, n_row), r + n_row * a).wait_send()
            return carry

        lax.fori_loop(1, n_row, z_done, 0)
    for b in range(t_cols):
        @pl.when(need_back(r, c + n_col * b))
        def _():
            each_col_copy(b, sent, False)

        each_x_copy(b, sent)


def per_device(
    root_rhs, diag_inv, tile_u, tile_v, tile_rank, child_x, border_t, child_inv, child_blocks
):
    n_row = lax.axis_size("row")
    n_col = lax.axis_size("col")
    ntile, tile = diag_inv.shape[0], diag_inv.shape[1]
    rhs_count = root_rhs.shape[0]
    t_rows, t_cols, rank_max = tile_u.shape[2], tile_u.shape[3], tile_u.shape[4]
    n_child, bb = child_blocks.shape
    share = ntile * tile // (n_row * n_col)
    width = share if share % BLK == 0 else BLK
    vec = (rhs_count, tile)
    any_spec = pl.BlockSpec(memory_space=pl.ANY)
    vmem = pl.BlockSpec(memory_space=pltpu.VMEM)
    smem = pl.BlockSpec(memory_space=pltpu.SMEM)
    dma = pltpu.SemaphoreType.DMA
    root, child = pl.pallas_call(
        functools.partial(
            solve_kernel, n_row, n_col, t_rows, t_cols, ntile, n_child, bb, share
        ),
        out_shape=(
            jax.ShapeDtypeStruct((rhs_count, width), F32),
            jax.ShapeDtypeStruct(child_x.shape, F32),
        ),
        in_specs=[any_spec, any_spec, any_spec, any_spec, smem, vmem, any_spec, any_spec, smem],
        out_specs=(vmem, vmem),
        scratch_shapes=[
            pltpu.VMEM((t_rows,) + vec, BF16),
            pltpu.VMEM((t_rows, tile, tile), BF16),
            pltpu.VMEM((t_cols, tile, tile), BF16),
            pltpu.VMEM(tile_u.shape[2:], BF16),
            pltpu.VMEM(tile_v.shape[2:], BF16),
            pltpu.VMEM(border_t.shape, BF16),
            pltpu.VMEM(child_inv.shape, BF16),
            pltpu.VMEM((t_rows, t_cols, 2 * rank_max, tile), BF16),
            pltpu.VMEM((t_rows, t_cols, tile, 2 * rank_max), BF16),
            pltpu.VMEM((n_row, t_rows) + vec, F32),
            pltpu.VMEM((n_row, t_rows) + vec, F32),
            pltpu.VMEM((t_rows,) + vec, F32),
            pltpu.VMEM((t_cols, n_col) + vec, F32),
            pltpu.VMEM((t_cols, n_col) + vec, F32),
            pltpu.VMEM((t_cols,) + vec, F32),
            pltpu.VMEM((t_cols,) + vec, F32),
            pltpu.VMEM((t_rows, n_row) + vec, F32),
            pltpu.VMEM((t_rows, n_row) + vec, F32),
            pltpu.VMEM((ntile * tile // BLK, rhs_count, BLK), F32),
            pltpu.VMEM((t_rows, tile, rank_max), F32),
            pltpu.VMEM((t_rows, rank_max, tile), F32),
            pltpu.VMEM((t_rows, rank_max, tile), F32),
            pltpu.VMEM((t_rows, tile, rank_max), F32),
            pltpu.VMEM((t_cols, tile, rank_max), F32),
            pltpu.VMEM((t_cols, rank_max, tile), F32),
            pltpu.VMEM((t_rows, rank_max, tile), F32),
            pltpu.VMEM((t_rows, tile, rank_max), F32),
            pltpu.VMEM((tile, rank_max), BF16),
            pltpu.VMEM((2 * rank_max, tile), BF16),
            pltpu.VMEM((rank_max, tile), BF16),
            pltpu.VMEM((tile, 2 * rank_max), BF16),
            dma((4 + 2 * t_rows + t_cols,)),
            dma((n_row,)),
            dma((n_row,)),
            dma((t_rows, n_row)),
            dma((t_cols, n_col)),
            dma((t_rows, 2)),
            dma((t_cols, n_col)),
            dma((t_cols, n_col)),
            dma((t_rows, n_row)),
            dma((t_cols, 2)),
            dma((t_rows, n_row)),
            dma((t_cols, n_row)),
            dma((t_cols,)),
            dma((t_rows, n_row)),
            dma((ntile,)),
            dma((t_rows, n_col)),
            dma((t_rows, 2, 2)),
            dma((t_cols, 2)),
            dma((t_rows, 2, 2)),
            dma((t_rows, 2)),
        ],
        compiler_params=pltpu.CompilerParams(collective_id=0, has_side_effects=True),
    )(
        root_rhs, diag_inv, tile_u[0, 0], tile_v[0, 0], tile_rank[0, 0],
        child_x, border_t, child_inv, child_blocks,
    )
    if width != share:
        me = lax.axis_index("row") * n_col + lax.axis_index("col")
        root = lax.dynamic_slice_in_dim(root, (me * share) % BLK, share, 1)
    return root, child


def solution(mesh):
    return jax.shard_map(
        per_device,
        mesh=mesh,
        in_specs=(
            P(),
            P(),
            P("row", "col", None, None, None, None),
            P("row", "col", None, None, None, None),
            P("row", "col", None, None),
            P(("row", "col"), None, None),
            P(("row", "col"), None, None),
            P(("row", "col"), None, None),
            P(("row", "col"), None),
        ),
        out_specs=(P(None, ("row", "col")), P(("row", "col"), None, None)),
        check_vma=False,
    )
```
